32 devices in a mesh: seq: 4 (over y, x), blk: 8 (over z, core).
Axes of the slice: x: 2, y: 2, z: 4, core: 2. Of those that a mesh axis runs over, the one named last changes fastest.
Arguments:
- queries: bfloat16 [4, 2048, 2048], P('seq', 'blk'), may hold values from -150 to 150
- keys: bfloat16 [4, 256, 2048], P('seq', 'blk'), may hold values from -6 to 6
- values: bfloat16 [4, 256, 2048], P('seq', 'blk'), may hold values from -6 to 6
- image_index: int32 [4, 2048], P('seq', 'blk'), may hold values from 0 to 3, as said below
- head_gate: float32 [16], replicated, may hold values from 0.3 to 1.5
- out_weight: bfloat16 [2048, 4096], P(None, 'blk'), may hold values from -0.125 to 0.125
Outputs:
- layer_out: bfloat16 [4, 2048, 4096], P('seq', 'blk')
The draws below stay inside these ranges and needn't reach their ends.
Inputs may be any that keep to these rules, and one draw needn't show every extreme that they name: Along each sequence image_index never falls; each image's run of text tokens is at least 256 long, so one device's tokens meet at most two images.
All inputs are finite; a program needn't handle non-finite values.
Results may differ from the reference program's by a relative error of at most 0.008.
Values may be sent and summed in bfloat16 or wider, within the bound.
A program may use at most 128 MiB of HBM per device.

```python
import jax
import jax.numpy as jnp
from jax import lax

D = 4096
HEADS = 16
HD = 128
IMAGES = 4
TOK_DEV = 256
HQ = 2048
SEQS = 4
TEXT = 2048
LATENTS = 256
LAT_IMG = 64
TXT_IMG = 512


def image_layout(key):
    offsets = jax.random.randint(jax.random.fold_in(key, 11), (SEQS, IMAGES - 1), -(TXT_IMG // 4), TXT_IMG // 4 + 1)
    bounds = offsets + TXT_IMG * jnp.arange(1, IMAGES, dtype=jnp.int32)[None, :]
    positions = jnp.arange(TEXT, dtype=jnp.int32)
    return jnp.sum((positions[None, :, None] >= bounds[:, None, :]).astype(jnp.int32), axis=2)


def latent_keys(key):
    base = jax.random.truncated_normal(jax.random.fold_in(key, 22), -6.0, 6.0, (SEQS, LATENTS, HEADS * HD), jnp.float32)
    return base


def draw_keys(key, part):
    return latent_keys(key).astype(jnp.bfloat16)


def draw_queries(key, part):
    base = jax.random.truncated_normal(jax.random.fold_in(key, 33), -6.0, 6.0, (SEQS, TEXT, HEADS * HD), jnp.float32)
    return base.astype(jnp.bfloat16)


def draw_image_index(key, part):
    return image_layout(key)


def block_scale(own_key, dims, pieces, low, high):
    loudness = 1.0
    for axis_at, blocks in pieces:
        draws = jax.random.uniform(jax.random.fold_in(jax.random.fold_in(own_key, 6), axis_at), (blocks,), jnp.float32, low / len(pieces), high / len(pieces))
        loudness = loudness * jnp.repeat(jnp.exp(draws), dims[axis_at] // blocks).reshape((-1,) + (1,) * (len(dims) - 1 - axis_at))
    return loudness


def scatter_about(rng, extent, scale, bound, shards=(), held_as=jnp.bfloat16):
    drawn = scale * jax.random.normal(rng, extent, jnp.float32)
    if shards:
        drawn = drawn * block_scale(rng, extent, shards, -0.22, 0.18)
    return jnp.clip(drawn, -bound, bound).astype(held_as)


def setup_inputs(seed: int = 0) -> dict:
    arg_keys = jax.random.split(jax.random.key(seed), 7)
    queries = draw_queries(jax.random.fold_in(arg_keys[6], 71), 0)
    keys = draw_keys(jax.random.fold_in(arg_keys[6], 71), 0)
    values = scatter_about(arg_keys[2], (SEQS, LATENTS, HQ), 1.0, 6.0, ((0, 4), (1, 8)))
    image_index = draw_image_index(jax.random.fold_in(arg_keys[6], 71), 0)
    head_gate = jnp.clip(jax.random.uniform(arg_keys[4], (HEADS,), jnp.float32, 0.3, 1.5), 0.3, 1.5)
    out_weight = scatter_about(arg_keys[5], (HQ, D), HQ ** -0.5, 0.125, ((1, 8),))
    return dict(queries=queries, keys=keys, values=values, image_index=image_index, head_gate=head_gate, out_weight=out_weight)


def reference(queries, keys, values, image_index, head_gate, out_weight):
    heads = head_gate.shape[0]
    head_size = queries.shape[2] // heads
    scaling = head_size ** -0.5
    latent_image = jnp.arange(LATENTS, dtype=jnp.int32) // LAT_IMG
    gate_value = jnp.tanh(head_gate.astype(jnp.float32))

    def one_sequence(seq_args):
        query_seq, key_seq, value_seq, image_seq = seq_args
        key_heads = key_seq.astype(jnp.float32).reshape(LATENTS, heads, head_size)
        value_heads = value_seq.astype(jnp.float32).reshape(LATENTS, heads, head_size)

        def one_block(block_args):
            query_block, image_block = block_args
            query_heads = query_block.astype(jnp.float32).reshape(-1, heads, head_size)
            scores = jnp.einsum("thd,lhd->thl", query_heads, key_heads, precision=lax.Precision.HIGHEST) * scaling
            allowed = latent_image[None, None, :] <= image_block[:, None, None]
            largest = jnp.max(jnp.where(allowed, scores, -1e30), axis=2, keepdims=True)
            probs = jnp.exp(jnp.where(allowed, scores - largest, -1e30))
            denom = jnp.sum(probs, axis=2)
            rounded = lax.optimization_barrier(probs.astype(jnp.bfloat16)).astype(jnp.float32)
            weighted = jnp.einsum("thl,lhd->thd", rounded, value_heads, precision=lax.Precision.HIGHEST)
            attended = weighted / denom[:, :, None] * gate_value[None, :, None]
            hidden = attended.reshape(query_heads.shape[0], -1).astype(jnp.bfloat16)
            return jnp.dot(hidden, out_weight, preferred_element_type=jnp.float32).astype(jnp.bfloat16)

        blocks = lax.map(one_block, (query_seq.reshape(TEXT // TOK_DEV, TOK_DEV, -1),
                                     image_seq.reshape(TEXT // TOK_DEV, TOK_DEV)))
        return blocks.reshape(TEXT, -1)

    return lax.map(one_sequence, (queries, keys, values, image_index))
```

```python
import functools

import jax
import jax.numpy as jnp
from jax import lax
from jax.experimental import pallas as pl
from jax.experimental.pallas import tpu as pltpu
from jax.sharding import PartitionSpec as P

IMAGES = 4
QUARTERS = 4
CHUNK_BYTES = 128 * 1024
MESH = pl.DeviceIdType.MESH


def kernel(
    chips, parts, queries, keys, values, images, gate, weight, out,
    wbuf, qbuf, kbuf, vbuf, hidden, bias,
    load_sem, own_recv, own_send, wide_recv, side_recv, side_send, wide_send, down_send,
    kv_wide_recv, kv_side_recv, kv_wide_send, kv_down_send, kv_side_send,
):
    seq, blk = lax.axis_index("seq"), lax.axis_index("blk")
    chip, core = blk // 2, blk % 2
    quarter = seq % QUARTERS
    base = seq - quarter
    sibling = 2 * chip + 1 - core
    seq_x = base + jnp.where(quarter % 2 == 0, quarter + 1, quarter - 1)
    seq_y = base + (quarter + 2) % 4
    quarter_x, quarter_y = seq_x - base, seq_y - base
    quarter_d = jnp.where(quarter_x % 4 < 2, quarter_x + 2, quarter_x - 2)
    quarter_of = (quarter, quarter_x, quarter_y, quarter_d)
    rows = weight.shape[0] // QUARTERS
    step_rows = rows // parts
    lat_rows = keys.shape[0]
    width = weight.shape[1]
    tok_rows = qbuf.shape[0]

    def send(src, send_sem, recv_sem, seq_to, blk_to):
        return pltpu.make_async_remote_copy(
            src_ref=src, dst_ref=src, send_sem=send_sem, recv_sem=recv_sem,
            device_id=(seq_to, blk_to), device_id_type=MESH,
        )

    def piece(block, kind, part):
        start = pl.multiple_of(quarter_of[kind] * rows + part * step_rows, step_rows)
        return wbuf.at[block, pl.ds(start, step_rows), :]

    def lat(buf, block):
        return buf.at[pl.ds(pl.multiple_of(block * lat_rows, lat_rows), lat_rows), :]

    loads = [
        pltpu.make_async_copy(weight, wbuf.at[blk], load_sem.at[0]),
        pltpu.make_async_copy(keys, lat(kbuf, blk), load_sem.at[1]),
        pltpu.make_async_copy(values, lat(vbuf, blk), load_sem.at[2]),
        pltpu.make_async_copy(queries, qbuf, load_sem.at[3]),
    ]
    for load in loads:
        load.start()

    barrier = pltpu.get_barrier_semaphore()
    for seq_to, blk_to in ((seq, sibling), (seq_x, blk), (seq_y, blk)):
        pl.semaphore_signal(barrier, inc=1, device_id=(seq_to, blk_to), device_id_type=MESH)

    @pl.when(chip > 0)
    def _():
        pl.semaphore_signal(barrier, inc=1, device_id=(seq, blk - 2), device_id_type=MESH)

    @pl.when(chip < chips - 1)
    def _():
        pl.semaphore_signal(barrier, inc=1, device_id=(seq, blk + 2), device_id_type=MESH)

    pl.semaphore_wait(
        barrier, 3 + (chip > 0).astype(jnp.int32) + (chip < chips - 1).astype(jnp.int32)
    )
    for load in loads[:3]:
        load.wait()

    kv_bufs = (kbuf, vbuf)

    def own_wide(part, up):
        at = chip * parts + part
        sem = wide_send.at[0, at] if up else down_send.at[part]
        return send(piece(blk, 0, part), sem, wide_recv.at[0, at], seq, blk + 2 if up else blk - 2)

    def own_kv(which, up):
        sem = kv_wide_send.at[which, chip] if up else kv_down_send.at[which]
        return send(
            lat(kv_bufs[which], blk), sem, kv_wide_recv.at[which, chip], seq,
            blk + 2 if up else blk - 2,
        )

    own_side = send(wbuf.at[blk], own_send.at[0], own_recv.at[0], seq, sibling)

    def side_kv(which, block_chip):
        block = 2 * block_chip + core
        return send(
            lat(kv_bufs[which], block), kv_side_send.at[which, block_chip],
            kv_side_recv.at[which, block_chip], seq, sibling,
        )

    def for_own(act):
        early = max(parts - 1, 1)
        for part in range(early):
            act(lambda up, part=part: own_wide(part, up))
        for which in range(2):
            act(lambda up, which=which: own_kv(which, up))
        for part in range(early, parts):
            act(lambda up, part=part: own_wide(part, up))

    @pl.when(chip < chips - 1)
    def _():
        for_own(lambda make: make(True).start())

    @pl.when(chip > 0)
    def _():
        for_own(lambda make: make(False).start())

    own_side.start()
    for which in range(2):
        side_kv(which, chip).start()

    def wide(kind, block_chip, part):
        at = block_chip * parts + part
        return send(
            piece(2 * block_chip + core, kind, part), wide_send.at[kind, at],
            wide_recv.at[kind, at], seq, blk,
        )

    def onward(block_chip, part, up):
        at = block_chip * parts + part
        return send(
            piece(2 * block_chip + core, 0, part), wide_send.at[0, at], wide_recv.at[0, at],
            seq, blk + 2 if up else blk - 2,
        )

    def plane(kind, block_chip, part):
        at = block_chip * parts + part
        return send(
            piece(2 * block_chip + core, 0, part), wide_send.at[kind, at], wide_recv.at[kind, at],
            seq_x if kind == 1 else seq_y, blk,
        )

    def relay(kind, block_chip, part):
        at = block_chip * parts + part
        return send(
            piece(2 * block_chip + core, kind, part), wide_send.at[3, at], wide_recv.at[3, at],
            seq_y if kind == 1 else seq_x, blk,
        )

    def side(kind, block_chip, part, block_core=None):
        at = block_chip * parts + part
        block = 2 * block_chip + (core if block_core is None else block_core)
        return send(
            piece(block, kind, part), side_send.at[kind, at], side_recv.at[kind, at], seq, sibling,
        )

    def kv_onward(which, block_chip, up):
        return send(
            lat(kv_bufs[which], 2 * block_chip + core), kv_wide_send.at[which, block_chip],
            kv_wide_recv.at[which, block_chip], seq, blk + 2 if up else blk - 2,
        )

    def on_sides(distance, act):
        @pl.when(chip - distance >= 0)
        def _():
            act(chip - distance, True, chip < chips - 1)

        @pl.when(chip + distance < chips)
        def _():
            act(chip + distance, False, chip > 0)

    def line_step(distance, part):
        def act(block_chip, up, more):
            wide(0, block_chip, part).wait_recv()

            @pl.when(more)
            def _():
                onward(block_chip, part, up).start()

            plane(1, block_chip, part).start()
            plane(2, block_chip, part).start()
            side(0, block_chip, part).start()

        on_sides(distance, act)

    def relay_kind(step):
        return 1 + step % 2

    def plane_step(step, distance, part):
        def act(block_chip, up, more):
            for kind in (1, 2):
                wide(kind, block_chip, part).wait_recv()
                if kind == relay_kind(step):
                    relay(kind, block_chip, part).start()
                side(kind, block_chip, part).start()

        on_sides(distance, act)

    def corner_step(distance, part):
        def act(block_chip, up, more):
            wide(3, block_chip, part).wait_recv()
            side(3, block_chip, part).start()

        on_sides(distance, act)

    def kv_step(distance):
        def act(block_chip, up, more):
            for which in range(2):
                kv_onward(which, block_chip, up).wait_recv()

                @pl.when(more)
                def _():
                    kv_onward(which, block_chip, up).start()

                side_kv(which, block_chip).start()

        on_sides(distance, act)

    def attention():
        for block_chip in range(chips):
            for which in range(2):
                side_kv(which, block_chip).wait_recv()
        loads[3].wait()
        count = kbuf.shape[0]
        image_rows = count // IMAGES
        image_lanes = jnp.transpose(jnp.broadcast_to(images[...], (128, tok_rows)))
        for tile in range(count // 128):
            lane = tile * 128 + lax.broadcasted_iota(jnp.int32, (tok_rows, 128), 1)
            bias[:, tile * 128 : (tile + 1) * 128] = jnp.where(
                lane // image_rows <= image_lanes, 0.0, -1e30
            )
        heads = gate.shape[0]
        head_size = qbuf.shape[1] // heads

        @pl.loop(0, heads)
        def _(head):
            cols = pl.ds(pl.multiple_of(head * head_size, head_size), head_size)
            scores = lax.dot_general(
                qbuf[:, cols], kbuf[:, cols], (((1,), (1,)), ((), ())),
                preferred_element_type=jnp.float32,
            ) * head_size ** (-0.5) + bias[...]
            largest = jnp.max(scores, axis=1, keepdims=True)
            probs = jnp.exp(scores - largest)
            denom = jnp.sum(probs, axis=1, keepdims=True)
            weighted = jnp.dot(
                probs.astype(jnp.bfloat16), vbuf[:, cols], preferred_element_type=jnp.float32
            )
            gate_value = jnp.tanh(jnp.full((1, head_size), gate[head], jnp.float32))
            hidden[:, cols] = (weighted / denom * gate_value).astype(jnp.bfloat16)

    def project(block):
        out[:, pl.ds(pl.multiple_of(block * width, width), width)] = jnp.dot(
            hidden[...], wbuf[block], preferred_element_type=jnp.float32
        ).astype(out.dtype)

    def project_own():
        own_side.wait_recv()

        @pl.loop(0, 2)
        def _(at):
            project(2 * chip + at)

    def project_distance(distance):
        def act(block_chip, up, more):
            for part in range(parts):
                for kind in range(4):
                    side(kind, block_chip, part, 1 - core).wait_recv()

            @pl.loop(0, 2)
            def _(at):
                project(2 * block_chip + at)

        on_sides(distance, act)

    steps = [(distance, part) for distance in range(1, chips) for part in range(parts)]
    total = len(steps)
    kv_at = [min(total - 1, distance * parts * 2 // 3) for distance in range(1, chips)]
    work = [attention, project_own]
    for step in range(total + 2):
        if step < total:
            line_step(*steps[step])
        if 1 <= step <= total:
            plane_step(step - 1, *steps[step - 1])
        if step >= 2:
            corner_step(*steps[step - 2])
            if steps[step - 2][1] == parts - 1:
                work.append(functools.partial(project_distance, steps[step - 2][0]))
        for distance in range(1, chips):
            if kv_at[distance - 1] == step:
                kv_step(distance)
        if step >= kv_at[-1] and work:
            work.pop(0)()
    for task in work:
        task()

    @pl.when(chip < chips - 1)
    def _():
        for_own(lambda make: make(True).wait_send())

    @pl.when(chip > 0)
    def _():
        for_own(lambda make: make(False).wait_send())

    own_side.wait_send()
    for which in range(2):
        side_kv(which, chip).wait_send()
    for step in range(total):
        distance, part = steps[step]

        def act(block_chip, up, more):
            @pl.when(more)
            def _():
                onward(block_chip, part, up).wait_send()

            plane(1, block_chip, part).wait_send()
            plane(2, block_chip, part).wait_send()
            relay(relay_kind(step), block_chip, part).wait_send()
            for kind in range(4):
                side(kind, block_chip, part).wait_send()

        on_sides(distance, act)
    for distance in range(1, chips):

        def act(block_chip, up, more):
            for which in range(2):

                @pl.when(more)
                def _():
                    kv_onward(which, block_chip, up).wait_send()

                side_kv(which, block_chip).wait_send()

        on_sides(distance, act)


def per_device(queries, keys, values, image_index, head_gate, out_weight):
    blocks = lax.axis_size("blk")
    chips = blocks // 2
    tok_rows, features = queries.shape[1:]
    latents = keys.shape[1] * blocks
    depth, width = out_weight.shape
    parts = max(1, depth * width * 2 // QUARTERS // CHUNK_BYTES)
    pieces = chips * parts
    dma = pltpu.SemaphoreType.DMA
    anywhere = pl.BlockSpec(memory_space=pl.ANY)
    result = pl.pallas_call(
        functools.partial(kernel, chips, parts),
        out_shape=jax.ShapeDtypeStruct((tok_rows, width * blocks), jnp.bfloat16),
        in_specs=[
            anywhere, anywhere, anywhere,
            pl.BlockSpec(memory_space=pltpu.VMEM),
            pl.BlockSpec(memory_space=pltpu.SMEM),
            anywhere,
        ],
        out_specs=pl.BlockSpec(memory_space=pltpu.VMEM),
        scratch_shapes=[
            pltpu.VMEM((blocks, depth, width), jnp.bfloat16),
            pltpu.VMEM((tok_rows, features), jnp.bfloat16),
            pltpu.VMEM((latents, features), jnp.bfloat16),
            pltpu.VMEM((latents, features), jnp.bfloat16),
            pltpu.VMEM((tok_rows, features), jnp.bfloat16),
            pltpu.VMEM((tok_rows, latents), jnp.float32),
            dma((4,)), dma((1,)), dma((1,)),
            dma((4, pieces)), dma((4, pieces)), dma((4, pieces)), dma((4, pieces)), dma((parts,)),
            dma((2, chips)), dma((2, chips)), dma((2, chips)), dma((2,)), dma((2, chips)),
        ],
        compiler_params=pltpu.CompilerParams(
            collective_id=0, has_side_effects=True, vmem_limit_bytes=60000 * 1024
        ),
    )(queries[0], keys[0], values[0], image_index, head_gate, out_weight)
    return result[None]


def solution(mesh):
    placed = (
        P("seq", "blk", None),
        P("seq", "blk", None),
        P("seq", "blk", None),
        P("seq", "blk"),
        P(),
        P(None, "blk"),
    )
    return jax.shard_map(
        per_device, mesh=mesh, in_specs=placed, out_specs=P("seq", "blk", None), check_vma=False
    )
```

```python
import functools

import jax
import jax.numpy as jnp
from jax import lax
from jax.experimental import pallas as pl
from jax.experimental.pallas import tpu as pltpu
from jax.sharding import PartitionSpec as P

IMAGES = 4
QUARTERS = 4
CHUNK_BYTES = 256 * 1024
LAG = 1
MESH = pl.DeviceIdType.MESH


def kernel(
    chips, parts, queries, keys, values, images, gate, weight, out,
    wbuf, qbuf, kbuf, vbuf, hidden, bias,
    load_sem, own_recv, own_send, wide_recv, side_recv, side_send, wide_send, down_send,
    relay_recv, relay_send,
    kv_wide_recv, kv_side_recv, kv_wide_send, kv_down_send, kv_side_send,
):
    seq, blk = lax.axis_index("seq"), lax.axis_index("blk")
    chip, core = blk // 2, blk % 2
    quarter = seq % QUARTERS
    base = seq - quarter
    sibling = 2 * chip + 1 - core
    seq_x = base + jnp.where(quarter % 2 == 0, quarter + 1, quarter - 1)
    seq_y = base + (quarter + 2) % 4
    quarter_x, quarter_y = seq_x - base, seq_y - base
    quarter_d = jnp.where(quarter_x % 4 < 2, quarter_x + 2, quarter_x - 2)
    quarter_of = (quarter, quarter_x, quarter_y, quarter_d)
    rows = weight.shape[0] // QUARTERS
    step_rows = rows // parts
    lat_rows = keys.shape[0]
    width = weight.shape[1]
    tok_rows = qbuf.shape[0]

    def send(src, send_sem, recv_sem, seq_to, blk_to):
        return pltpu.make_async_remote_copy(
            src_ref=src, dst_ref=src, send_sem=send_sem, recv_sem=recv_sem,
            device_id=(seq_to, blk_to), device_id_type=MESH,
        )

    def piece(block, kind, part):
        start = pl.multiple_of(quarter_of[kind] * rows + part * step_rows, step_rows)
        return wbuf.at[block, pl.ds(start, step_rows), :]

    def lat(buf, block):
        return buf.at[pl.ds(pl.multiple_of(block * lat_rows, lat_rows), lat_rows), :]

    loads = [
        pltpu.make_async_copy(weight, wbuf.at[blk], load_sem.at[0]),
        pltpu.make_async_copy(keys, lat(kbuf, blk), load_sem.at[1]),
        pltpu.make_async_copy(values, lat(vbuf, blk), load_sem.at[2]),
        pltpu.make_async_copy(queries, qbuf, load_sem.at[3]),
    ]
    for load in loads:
        load.start()

    barrier = pltpu.get_barrier_semaphore()
    for seq_to, blk_to in ((seq, sibling), (seq_x, blk), (seq_y, blk)):
        pl.semaphore_signal(barrier, inc=1, device_id=(seq_to, blk_to), device_id_type=MESH)

    @pl.when(chip > 0)
    def _():
        pl.semaphore_signal(barrier, inc=1, device_id=(seq, blk - 2), device_id_type=MESH)

    @pl.when(chip < chips - 1)
    def _():
        pl.semaphore_signal(barrier, inc=1, device_id=(seq, blk + 2), device_id_type=MESH)

    pl.semaphore_wait(
        barrier, 3 + (chip > 0).astype(jnp.int32) + (chip < chips - 1).astype(jnp.int32)
    )
    for load in loads[:3]:
        load.wait()

    kv_bufs = (kbuf, vbuf)

    def own_wide(part, up):
        at = chip * parts + part
        sem = wide_send.at[0, at] if up else down_send.at[part]
        return send(piece(blk, 0, part), sem, wide_recv.at[0, at], seq, blk + 2 if up else blk - 2)

    def own_kv(which, up):
        sem = kv_wide_send.at[which, chip] if up else kv_down_send.at[which]
        return send(
            lat(kv_bufs[which], blk), sem, kv_wide_recv.at[which, chip], seq,
            blk + 2 if up else blk - 2,
        )

    own_side = send(wbuf.at[blk], own_send.at[0], own_recv.at[0], seq, sibling)

    def side_kv(which, block_chip):
        block = 2 * block_chip + core
        return send(
            lat(kv_bufs[which], block), kv_side_send.at[which, block_chip],
            kv_side_recv.at[which, block_chip], seq, sibling,
        )

    def for_own(act):
        early = max(parts - 1, 1)
        for part in range(early):
            act(lambda up, part=part: own_wide(part, up))
        for which in range(2):
            act(lambda up, which=which: own_kv(which, up))
        for part in range(early, parts):
            act(lambda up, part=part: own_wide(part, up))

    @pl.when(chip < chips - 1)
    def _():
        for_own(lambda make: make(True).start())

    @pl.when(chip > 0)
    def _():
        for_own(lambda make: make(False).start())

    own_side.start()
    for which in range(2):
        side_kv(which, chip).start()

    def wide(kind, block_chip, part):
        at = block_chip * parts + part
        return send(
            piece(2 * block_chip + core, kind, part), wide_send.at[kind, at],
            wide_recv.at[kind, at], seq, blk,
        )

    def onward(block_chip, part, up):
        at = block_chip * parts + part
        return send(
            piece(2 * block_chip + core, 0, part), wide_send.at[0, at], wide_recv.at[0, at],
            seq, blk + 2 if up else blk - 2,
        )

    def plane(kind, block_chip, part):
        at = block_chip * parts + part
        return send(
            piece(2 * block_chip + core, 0, part), wide_send.at[kind, at], wide_recv.at[kind, at],
            seq_x if kind == 1 else seq_y, blk,
        )

    def relay(kind, block_chip, part):
        at = block_chip * parts + part
        half = step_rows // 2
        src = piece(2 * block_chip + core, kind, part).at[pl.ds((kind - 1) * half, half), :]
        return send(
            src, relay_send.at[kind - 1, at], relay_recv.at[kind - 1, at],
            seq_y if kind == 1 else seq_x, blk,
        )

    def corner(kind, block_chip, part):
        at = block_chip * parts + part
        half = step_rows // 2
        dst = piece(2 * block_chip + core, 3, part).at[pl.ds((kind - 1) * half, half), :]
        return send(dst, relay_send.at[kind - 1, at], relay_recv.at[kind - 1, at], seq, blk)

    def side(kind, block_chip, part, block_core=None):
        at = block_chip * parts + part
        block = 2 * block_chip + (core if block_core is None else block_core)
        return send(
            piece(block, kind, part), side_send.at[kind, at], side_recv.at[kind, at], seq, sibling,
        )

    def kv_onward(which, block_chip, up):
        return send(
            lat(kv_bufs[which], 2 * block_chip + core), kv_wide_send.at[which, block_chip],
            kv_wide_recv.at[which, block_chip], seq, blk + 2 if up else blk - 2,
        )

    def on_sides(distance, act):
        @pl.when(chip - distance >= 0)
        def _():
            act(chip - distance, True, chip < chips - 1)

        @pl.when(chip + distance < chips)
        def _():
            act(chip + distance, False, chip > 0)

    def line_step(distance, part):
        def act(block_chip, up, more):
            wide(0, block_chip, part).wait_recv()

            @pl.when(more)
            def _():
                onward(block_chip, part, up).start()

            plane(1, block_chip, part).start()
            plane(2, block_chip, part).start()
            side(0, block_chip, part).start()

        on_sides(distance, act)

    def plane_step(distance, part):
        def act(block_chip, up, more):
            for kind in (1, 2):
                wide(kind, block_chip, part).wait_recv()
                relay(kind, block_chip, part).start()
                side(kind, block_chip, part).start()

        on_sides(distance, act)

    def corner_step(distance, part):
        def act(block_chip, up, more):
            for kind in (1, 2):
                corner(kind, block_chip, part).wait_recv()
            side(3, block_chip, part).start()

        on_sides(distance, act)

    def kv_step(distance):
        def act(block_chip, up, more):
            for which in range(2):
                kv_onward(which, block_chip, up).wait_recv()

                @pl.when(more)
                def _():
                    kv_onward(which, block_chip, up).start()

                side_kv(which, block_chip).start()

        on_sides(distance, act)

    def attention():
        for block_chip in range(chips):
            for which in range(2):
                side_kv(which, block_chip).wait_recv()
        loads[3].wait()
        count = kbuf.shape[0]
        image_rows = count // IMAGES
        image_lanes = jnp.transpose(jnp.broadcast_to(images[...], (128, tok_rows)))
        for tile in range(count // 128):
            lane = tile * 128 + lax.broadcasted_iota(jnp.int32, (tok_rows, 128), 1)
            bias[:, tile * 128 : (tile + 1) * 128] = jnp.where(
                lane // image_rows <= image_lanes, 0.0, -1e30
            )
        heads = gate.shape[0]
        head_size = qbuf.shape[1] // heads

        @pl.loop(0, heads)
        def _(head):
            cols = pl.ds(pl.multiple_of(head * head_size, head_size), head_size)
            scores = lax.dot_general(
                qbuf[:, cols], kbuf[:, cols], (((1,), (1,)), ((), ())),
                preferred_element_type=jnp.float32,
            ) * head_size ** (-0.5) + bias[...]
            largest = jnp.max(scores, axis=1, keepdims=True)
            probs = jnp.exp(scores - largest)
            denom = jnp.sum(probs, axis=1, keepdims=True)
            weighted = jnp.dot(
                probs.astype(jnp.bfloat16), vbuf[:, cols], preferred_element_type=jnp.float32
            )
            gate_value = jnp.tanh(jnp.full((1, head_size), gate[head], jnp.float32))
            hidden[:, cols] = (weighted / denom * gate_value).astype(jnp.bfloat16)

    def project(block):
        out[:, pl.ds(pl.multiple_of(block * width, width), width)] = jnp.dot(
            hidden[...], wbuf[block], preferred_element_type=jnp.float32
        ).astype(out.dtype)

    def project_own():
        own_side.wait_recv()

        @pl.loop(0, 2)
        def _(at):
            project(2 * chip + at)

    def project_distance(distance):
        def act(block_chip, up, more):
            for part in range(parts):
                for kind in range(4):
                    side(kind, block_chip, part, 1 - core).wait_recv()

            @pl.loop(0, 2)
            def _(at):
                project(2 * block_chip + at)

        on_sides(distance, act)

    steps = [(distance, part) for distance in range(1, chips) for part in range(parts)]
    total = len(steps)
    kv_at = [min(total - 1, distance * parts * 2 // 3) for distance in range(1, chips)]
    work = [attention, project_own]
    for step in range(total + LAG + 1):
        if step < total:
            line_step(*steps[step])
        near = step - LAG
        if 0 <= near < total:
            plane_step(*steps[near])
        far = near - 1
        if 0 <= far < total:
            corner_step(*steps[far])
            if steps[far][1] == parts - 1:
                work.append(functools.partial(project_distance, steps[far][0]))
        for distance in range(1, chips):
            if kv_at[distance - 1] == step:
                kv_step(distance)
        if step >= kv_at[-1] and work:
            work.pop(0)()
    for task in work:
        task()

    @pl.when(chip < chips - 1)
    def _():
        for_own(lambda make: make(True).wait_send())

    @pl.when(chip > 0)
    def _():
        for_own(lambda make: make(False).wait_send())

    own_side.wait_send()
    for which in range(2):
        side_kv(which, chip).wait_send()
    for step in range(total):
        distance, part = steps[step]

        def act(block_chip, up, more):
            @pl.when(more)
            def _():
                onward(block_chip, part, up).wait_send()

            plane(1, block_chip, part).wait_send()
            plane(2, block_chip, part).wait_send()
            for kind in (1, 2):
                relay(kind, block_chip, part).wait_send()
            for kind in range(4):
                side(kind, block_chip, part).wait_send()

        on_sides(distance, act)
    for distance in range(1, chips):

        def act(block_chip, up, more):
            for which in range(2):

                @pl.when(more)
                def _():
                    kv_onward(which, block_chip, up).wait_send()

                side_kv(which, block_chip).wait_send()

        on_sides(distance, act)


def per_device(queries, keys, values, image_index, head_gate, out_weight):
    blocks = lax.axis_size("blk")
    chips = blocks // 2
    tok_rows, features = queries.shape[1:]
    latents = keys.shape[1] * blocks
    depth, width = out_weight.shape
    parts = max(1, depth * width * 2 // QUARTERS // CHUNK_BYTES)
    pieces = chips * parts
    dma = pltpu.SemaphoreType.DMA
    anywhere = pl.BlockSpec(memory_space=pl.ANY)
    result = pl.pallas_call(
        functools.partial(kernel, chips, parts),
        out_shape=jax.ShapeDtypeStruct((tok_rows, width * blocks), jnp.bfloat16),
        in_specs=[
            anywhere, anywhere, anywhere,
            pl.BlockSpec(memory_space=pltpu.VMEM),
            pl.BlockSpec(memory_space=pltpu.SMEM),
            anywhere,
        ],
        out_specs=pl.BlockSpec(memory_space=pltpu.VMEM),
        scratch_shapes=[
            pltpu.VMEM((blocks, depth, width), jnp.bfloat16),
            pltpu.VMEM((tok_rows, features), jnp.bfloat16),
            pltpu.VMEM((latents, features), jnp.bfloat16),
            pltpu.VMEM((latents, features), jnp.bfloat16),
            pltpu.VMEM((tok_rows, features), jnp.bfloat16),
            pltpu.VMEM((tok_rows, latents), jnp.float32),
            dma((4,)), dma((1,)), dma((1,)),
            dma((3, pieces)), dma((4, pieces)), dma((4, pieces)), dma((3, pieces)), dma((parts,)),
            dma((2, pieces)), dma((2, pieces)),
            dma((2, chips)), dma((2, chips)), dma((2, chips)), dma((2,)), dma((2, chips)),
        ],
        compiler_params=pltpu.CompilerParams(
            collective_id=0, has_side_effects=True, vmem_limit_bytes=60000 * 1024
        ),
    )(queries[0], keys[0], values[0], image_index, head_gate, out_weight)
    return result[None]


def solution(mesh):
    placed = (
        P("seq", "blk", None),
        P("seq", "blk", None),
        P("seq", "blk", None),
        P("seq", "blk"),
        P(),
        P(None, "blk"),
    )
    return jax.shard_map(
        per_device, mesh=mesh, in_specs=placed, out_specs=P("seq", "blk", None), check_vma=False
    )
```

```python
import functools

import jax
import jax.numpy as jnp
from jax import lax
from jax.experimental import pallas as pl
from jax.experimental.pallas import tpu as pltpu
from jax.sharding import PartitionSpec as P

IMAGES = 4
QUARTERS = 4
CHUNK_BYTES = 256 * 1024
LAG = 1
MESH = pl.DeviceIdType.MESH


def kernel(
    chips, parts, queries, keys, values, images, gate, weight, out,
    wbuf, qbuf, kbuf, vbuf, hidden, bias,
    load_sem, own_recv, own_send, wide_recv, side_recv, side_send, wide_send, down_send,
    relay_recv, relay_send,
    kv_wide_recv, kv_side_recv, kv_wide_send, kv_down_send, kv_side_send,
):
    seq, blk = lax.axis_index("seq"), lax.axis_index("blk")
    chip, core = blk // 2, blk % 2
    quarter = seq % QUARTERS
    base = seq - quarter
    sibling = 2 * chip + 1 - core
    seq_x = base + jnp.where(quarter % 2 == 0, quarter + 1, quarter - 1)
    seq_y = base + (quarter + 2) % 4
    quarter_x, quarter_y = seq_x - base, seq_y - base
    quarter_d = jnp.where(quarter_x % 4 < 2, quarter_x + 2, quarter_x - 2)
    quarter_of = (quarter, quarter_x, quarter_y, quarter_d)
    rows = weight.shape[0] // QUARTERS
    step_rows = rows // parts
    lat_rows = keys.shape[0]
    width = weight.shape[1]
    tok_rows = qbuf.shape[0]

    def send(src, send_sem, recv_sem, seq_to, blk_to):
        return pltpu.make_async_remote_copy(
            src_ref=src, dst_ref=src, send_sem=send_sem, recv_sem=recv_sem,
            device_id=(seq_to, blk_to), device_id_type=MESH,
        )

    def piece(block, kind, part):
        start = pl.multiple_of(quarter_of[kind] * rows + part * step_rows, step_rows)
        return wbuf.at[block, pl.ds(start, step_rows), :]

    def lat(buf, block):
        return buf.at[pl.ds(pl.multiple_of(block * lat_rows, lat_rows), lat_rows), :]

    loads = [
        pltpu.make_async_copy(weight, wbuf.at[blk], load_sem.at[0]),
        pltpu.make_async_copy(keys, lat(kbuf, blk), load_sem.at[1]),
        pltpu.make_async_copy(values, lat(vbuf, blk), load_sem.at[2]),
        pltpu.make_async_copy(queries, qbuf, load_sem.at[3]),
    ]
    for load in loads:
        load.start()

    barrier = pltpu.get_barrier_semaphore()
    for seq_to, blk_to in ((seq, sibling), (seq_x, blk), (seq_y, blk)):
        pl.semaphore_signal(barrier, inc=1, device_id=(seq_to, blk_to), device_id_type=MESH)

    @pl.when(chip > 0)
    def _():
        pl.semaphore_signal(barrier, inc=1, device_id=(seq, blk - 2), device_id_type=MESH)

    @pl.when(chip < chips - 1)
    def _():
        pl.semaphore_signal(barrier, inc=1, device_id=(seq, blk + 2), device_id_type=MESH)

    pl.semaphore_wait(
        barrier, 3 + (chip > 0).astype(jnp.int32) + (chip < chips - 1).astype(jnp.int32)
    )
    for load in loads[:3]:
        load.wait()

    kv_bufs = (kbuf, vbuf)

    def own_wide(part, up):
        at = chip * parts + part
        sem = wide_send.at[0, at] if up else down_send.at[part]
        return send(piece(blk, 0, part), sem, wide_recv.at[0, at], seq, blk + 2 if up else blk - 2)

    def own_kv(which, up):
        sem = kv_wide_send.at[which, chip] if up else kv_down_send.at[which]
        return send(
            lat(kv_bufs[which], blk), sem, kv_wide_recv.at[which, chip], seq,
            blk + 2 if up else blk - 2,
        )

    own_side = send(wbuf.at[blk], own_send.at[0], own_recv.at[0], seq, sibling)

    def side_kv(which, block_chip):
        block = 2 * block_chip + core
        return send(
            lat(kv_bufs[which], block), kv_side_send.at[which, block_chip],
            kv_side_recv.at[which, block_chip], seq, sibling,
        )

    def for_own(act):
        early = max(parts - 1, 1)
        for part in range(early):
            act(lambda up, part=part: own_wide(part, up))
        for which in range(2):
            act(lambda up, which=which: own_kv(which, up))
        for part in range(early, parts):
            act(lambda up, part=part: own_wide(part, up))

    @pl.when(chip < chips - 1)
    def _():
        for_own(lambda make: make(True).start())

    @pl.when(chip > 0)
    def _():
        for_own(lambda make: make(False).start())

    own_side.start()
    for which in range(2):
        side_kv(which, chip).start()

    def wide(kind, block_chip, part):
        at = block_chip * parts + part
        return send(
            piece(2 * block_chip + core, kind, part), wide_send.at[kind, at],
            wide_recv.at[kind, at], seq, blk,
        )

    def onward(block_chip, part, up):
        at = block_chip * parts + part
        return send(
            piece(2 * block_chip + core, 0, part), wide_send.at[0, at], wide_recv.at[0, at],
            seq, blk + 2 if up else blk - 2,
        )

    def plane(kind, block_chip, part):
        at = block_chip * parts + part
        return send(
            piece(2 * block_chip + core, 0, part), wide_send.at[kind, at], wide_recv.at[kind, at],
            seq_x if kind == 1 else seq_y, blk,
        )

    def relay(kind, block_chip, part):
        at = block_chip * parts + part
        half = step_rows // 2
        src = piece(2 * block_chip + core, kind, part).at[pl.ds((kind - 1) * half, half), :]
        return send(
            src, relay_send.at[kind - 1, at], relay_recv.at[kind - 1, at],
            seq_y if kind == 1 else seq_x, blk,
        )

    def corner(kind, block_chip, part):
        at = block_chip * parts + part
        half = step_rows // 2
        dst = piece(2 * block_chip + core, 3, part).at[pl.ds((kind - 1) * half, half), :]
        return send(dst, relay_send.at[kind - 1, at], relay_recv.at[kind - 1, at], seq, blk)

    def side(kind, block_chip, part, block_core=None):
        at = block_chip * parts + part
        block = 2 * block_chip + (core if block_core is None else block_core)
        return send(
            piece(block, kind, part), side_send.at[kind, at], side_recv.at[kind, at], seq, sibling,
        )

    def kv_onward(which, block_chip, up):
        return send(
            lat(kv_bufs[which], 2 * block_chip + core), kv_wide_send.at[which, block_chip],
            kv_wide_recv.at[which, block_chip], seq, blk + 2 if up else blk - 2,
        )

    def on_sides(distance, act):
        @pl.when(chip - distance >= 0)
        def _():
            act(chip - distance, True, chip < chips - 1)

        @pl.when(chip + distance < chips)
        def _():
            act(chip + distance, False, chip > 0)

    def line_step(distance, part):
        def act(block_chip, up, more):
            wide(0, block_chip, part).wait_recv()

            @pl.when(more)
            def _():
                onward(block_chip, part, up).start()

            plane(1, block_chip, part).start()
            plane(2, block_chip, part).start()
            side(0, block_chip, part).start()

        on_sides(distance, act)

    def plane_step(distance, part):
        def act(block_chip, up, more):
            for kind in (1, 2):
                wide(kind, block_chip, part).wait_recv()
                relay(kind, block_chip, part).start()
                side(kind, block_chip, part).start()

        on_sides(distance, act)

    def corner_step(distance, part):
        def act(block_chip, up, more):
            for kind in (1, 2):
                corner(kind, block_chip, part).wait_recv()
            side(3, block_chip, part).start()

        on_sides(distance, act)

    def kv_step(distance):
        def act(block_chip, up, more):
            for which in range(2):
                kv_onward(which, block_chip, up).wait_recv()

                @pl.when(more)
                def _():
                    kv_onward(which, block_chip, up).start()

                side_kv(which, block_chip).start()

        on_sides(distance, act)

    def attention():
        for block_chip in range(chips):
            for which in range(2):
                side_kv(which, block_chip).wait_recv()
        loads[3].wait()
        count = kbuf.shape[0]
        image_rows = count // IMAGES
        image_lanes = jnp.transpose(jnp.broadcast_to(images[...], (128, tok_rows)))
        for tile in range(count // 128):
            lane = tile * 128 + lax.broadcasted_iota(jnp.int32, (tok_rows, 128), 1)
            bias[:, tile * 128 : (tile + 1) * 128] = jnp.where(
                lane // image_rows <= image_lanes, 0.0, -1e30
            )
        heads = gate.shape[0]
        head_size = qbuf.shape[1] // heads

        @pl.loop(0, heads)
        def _(head):
            cols = pl.ds(pl.multiple_of(head * head_size, head_size), head_size)
            scores = lax.dot_general(
                qbuf[:, cols], kbuf[:, cols], (((1,), (1,)), ((), ())),
                preferred_element_type=jnp.float32,
            ) * head_size ** (-0.5) + bias[...]
            largest = jnp.max(scores, axis=1, keepdims=True)
            probs = jnp.exp(scores - largest)
            denom = jnp.sum(probs, axis=1, keepdims=True)
            weighted = jnp.dot(
                probs.astype(jnp.bfloat16), vbuf[:, cols], preferred_element_type=jnp.float32
            )
            gate_value = jnp.tanh(jnp.full((1, head_size), gate[head], jnp.float32))
            hidden[:, cols] = (weighted / denom * gate_value).astype(jnp.bfloat16)

    def project(block):
        out[:, pl.ds(pl.multiple_of(block * width, width), width)] = jnp.dot(
            hidden[...], wbuf[block], preferred_element_type=jnp.float32
        ).astype(out.dtype)

    def project_own():
        own_side.wait_recv()

        @pl.loop(0, 2)
        def _(at):
            project(2 * chip + at)

    def project_distance(distance):
        def act(block_chip, up, more):
            for part in range(parts):
                for kind in range(4):
                    side(kind, block_chip, part, 1 - core).wait_recv()

            @pl.loop(0, 2)
            def _(at):
                project(2 * block_chip + at)

        on_sides(distance, act)

    steps = [(distance, part) for distance in range(1, chips) for part in range(parts)]
    total = len(steps)
    kv_at = [min(total - 1, distance * parts * 2 // 3 - 1) for distance in range(1, chips)]
    work = [attention, project_own]
    for step in range(total + LAG + 1):
        if step < total:
            line_step(*steps[step])
        near = step - LAG
        if 0 <= near < total:
            plane_step(*steps[near])
        far = near - 1
        if 0 <= far < total:
            corner_step(*steps[far])
            if steps[far][1] == parts - 1:
                work.append(functools.partial(project_distance, steps[far][0]))
        for distance in range(1, chips):
            if kv_at[distance - 1] == step:
                kv_step(distance)
        if step >= kv_at[-1] and work:
            work.pop(0)()
    for task in work:
        task()

    @pl.when(chip < chips - 1)
    def _():
        for_own(lambda make: make(True).wait_send())

    @pl.when(chip > 0)
    def _():
        for_own(lambda make: make(False).wait_send())

    own_side.wait_send()
    for which in range(2):
        side_kv(which, chip).wait_send()
    for step in range(total):
        distance, part = steps[step]

        def act(block_chip, up, more):
            @pl.when(more)
            def _():
                onward(block_chip, part, up).wait_send()

            plane(1, block_chip, part).wait_send()
            plane(2, block_chip, part).wait_send()
            for kind in (1, 2):
                relay(kind, block_chip, part).wait_send()
            for kind in range(4):
                side(kind, block_chip, part).wait_send()

        on_sides(distance, act)
    for distance in range(1, chips):

        def act(block_chip, up, more):
            for which in range(2):

                @pl.when(more)
                def _():
                    kv_onward(which, block_chip, up).wait_send()

                side_kv(which, block_chip).wait_send()

        on_sides(distance, act)


def per_device(queries, keys, values, image_index, head_gate, out_weight):
    blocks = lax.axis_size("blk")
    chips = blocks // 2
    tok_rows, features = queries.shape[1:]
    latents = keys.shape[1] * blocks
    depth, width = out_weight.shape
    parts = max(1, depth * width * 2 // QUARTERS // CHUNK_BYTES)
    pieces = chips * parts
    dma = pltpu.SemaphoreType.DMA
    anywhere = pl.BlockSpec(memory_space=pl.ANY)
    result = pl.pallas_call(
        functools.partial(kernel, chips, parts),
        out_shape=jax.ShapeDtypeStruct((tok_rows, width * blocks), jnp.bfloat16),
        in_specs=[
            anywhere, anywhere, anywhere,
            pl.BlockSpec(memory_space=pltpu.VMEM),
            pl.BlockSpec(memory_space=pltpu.SMEM),
            anywhere,
        ],
        out_specs=pl.BlockSpec(memory_space=pltpu.VMEM),
        scratch_shapes=[
            pltpu.VMEM((blocks, depth, width), jnp.bfloat16),
            pltpu.VMEM((tok_rows, features), jnp.bfloat16),
            pltpu.VMEM((latents, features), jnp.bfloat16),
            pltpu.VMEM((latents, features), jnp.bfloat16),
            pltpu.VMEM((tok_rows, features), jnp.bfloat16),
            pltpu.VMEM((tok_rows, latents), jnp.float32),
            dma((4,)), dma((1,)), dma((1,)),
            dma((3, pieces)), dma((4, pieces)), dma((4, pieces)), dma((3, pieces)), dma((parts,)),
            dma((2, pieces)), dma((2, pieces)),
            dma((2, chips)), dma((2, chips)), dma((2, chips)), dma((2,)), dma((2, chips)),
        ],
        compiler_params=pltpu.CompilerParams(
            collective_id=0, has_side_effects=True, vmem_limit_bytes=60000 * 1024
        ),
    )(queries[0], keys[0], values[0], image_index, head_gate, out_weight)
    return result[None]


def solution(mesh):
    placed = (
        P("seq", "blk", None),
        P("seq", "blk", None),
        P("seq", "blk", None),
        P("seq", "blk"),
        P(),
        P(None, "blk"),
    )
    return jax.shard_map(
        per_device, mesh=mesh, in_specs=placed, out_specs=P("seq", "blk", None), check_vma=False
    )
```
